32 devices in a mesh: dp: 4 (over y, x), expert: 8 (over z, core).
Axes of the slice: x: 2, y: 2, z: 4, core: 2. Of those that a mesh axis runs over, the one named last changes fastest.
Arguments:
- tokens: bfloat16 [10240, 2048], P(('dp', 'expert')), may hold values from -6 to 6
- out_grad: bfloat16 [10240, 2048], P(('dp', 'expert')), may hold values from -6 to 6
- expert_ids: int32 [10240, 2], P(('dp', 'expert')), may hold values from 0 to 7, all different within a row; in each aligned block of 320 rows (0 to 319, 320 to 639, ...) at most 120 rows name the same one
- route_weight: bfloat16 [10240, 2], P(('dp', 'expert')), may hold values from 0.099609375 to 1
- w_gate: bfloat16 [8, 2048, 768], P('expert', 'dp'), may hold values from -0.125 to 0.125
- w_up: bfloat16 [8, 2048, 768], P('expert', 'dp'), may hold values from -0.125 to 0.125
- w_down: bfloat16 [8, 768, 2048], P('expert', None, 'dp'), may hold values from -0.21875 to 0.21875
Outputs:
- token_grad: bfloat16 [10240, 2048], P(('dp', 'expert'))
- route_grad: bfloat16 [10240, 2], P(('dp', 'expert'))
- gate_grad: bfloat16 [8, 2048, 768], P('expert', 'dp')
- up_grad: bfloat16 [8, 2048, 768], P('expert', 'dp')
- down_grad: bfloat16 [8, 768, 2048], P('expert', None, 'dp')
The draws below stay inside these ranges and needn't reach their ends.
Inputs may be any that keep to these rules, and one draw needn't show every extreme that they name: `expert_ids`: each row names 2 different experts. In the rows of one device no expert is named more than 120 times, a bound that some block reaches in some device.
All inputs are finite; a program needn't handle non-finite values.
Results may differ from the reference program's by a relative error of at most 0.014.
Values may be sent and summed in bfloat16 or wider, within the bound.
No kernel may reach another device: no remote copies, remote signals or barrier semaphores. Data moves between devices by JAX's collectives and lax.ppermute only.
A program may use at most 128 MiB of HBM per device.

```python
import math
import jax
import jax.numpy as jnp
import numpy as np
from jax import lax

D = 2048
FF = 768
TOP_WIN = 2
TOK_DEV = 320
EXPERTS_WIN = 8
CAP = 120
TOKENS = 10240
N_DP = 4
N_EXPERT = 8


def with_spikes(result, key, source, target, blocks, factor):
    owner, partner = [(jnp.arange(result.shape[axis_at]) // (result.shape[axis_at] // blocks)).reshape([-1 if axis == axis_at else 1 for axis in range(result.ndim)]) for axis_at in (source, target)]
    chosen = jax.random.permutation(key, blocks)[partner]
    strong = (owner == chosen) | (owner == (partner + blocks // 2) % blocks)
    return jnp.where(strong, factor * result, result)


def steps_of(rng, shape, pieces, smallest, largest):
    loudness = 1.0
    for dim, shards_of in pieces:
        heights = jax.random.uniform(jax.random.fold_in(jax.random.fold_in(rng, 6), dim), (shards_of,), jnp.float32, smallest / len(pieces), largest / len(pieces))
        loudness = loudness * jnp.repeat(jnp.exp(heights), shape[dim] // shards_of).reshape((-1,) + (1,) * (len(shape) - 1 - dim))
    return loudness


def routed_block(rng, own, number, rows, number_of, top, limit, slope):
    order = jax.random.permutation(rng, number_of)
    heavy_load, common = portions_of(number_of, rows * top, limit, slope, True), portions_of(number_of, rows * top, limit, slope, False)
    places = jnp.arange(number_of)

    def named(tallies, offset_by):
        used = int((tallies > 0).sum())
        fixed = max(1, used // 4)
        shifted = fixed + (places - fixed + offset_by * (used - fixed)) % max(1, number_of - fixed)
        return jnp.zeros((number_of,), jnp.int32).at[order[jnp.where(places < fixed, places, shifted)]].set(jnp.asarray(tallies, jnp.int32))

    tallies = jnp.where(number % 4 == 0, named(heavy_load, number // 4), named(common, number - number // 4 - 1))
    mixed = jax.random.permutation(jax.random.fold_in(own, 3), number_of)
    donor, taker = mixed[0:number_of // 2 * 2:2], mixed[1:number_of // 2 * 2:2]
    slack = jnp.minimum(tallies[donor] - 1, limit - tallies[taker]) // 2
    slack = jnp.where((donor == order[0]) | (taker == order[0]) | (tallies[taker] == 0), 0, jnp.maximum(slack, 0))
    shifted = jax.random.randint(jax.random.fold_in(own, 4), (number_of // 2,), 0, 1 << 20) % (slack + 1)
    tallies = tallies.at[donor].add(-shifted).at[taker].add(shifted)
    members = jnp.searchsorted(jnp.cumsum(tallies), jnp.arange(rows * top), side="right").astype(jnp.int32)
    listing = members.reshape(top, rows).T
    listing = listing[jax.random.permutation(jax.random.fold_in(own, 1), rows)]
    offset_by = jax.random.randint(jax.random.fold_in(own, 2), (rows, 1), 0, top)
    return jnp.take_along_axis(listing, (jnp.arange(top)[None, :] + offset_by) % top, axis=1)


def portions_of(count, total, most, lean, full):
    loads = [(1 << 20) // math.isqrt(standing ** lean) + 1 for standing in range(1, count + 1)]
    largest = most if full else min(most, max(-(-total // count), total * loads[0] // sum(loads)))
    least = 1 if total - largest >= count - 1 else 0
    given, rest = [largest] + [least] * (count - 1), total - largest - least * (count - 1)
    while rest > 0:
        movable = [i for i in range(1, count) if given[i] < largest] or [i for i in range(1, count) if given[i] < most]
        pool, left = sum([loads[i] for i in movable]), rest
        for i in movable:
            more = min(most - given[i], max(1, left * loads[i] // pool), rest)
            given[i] = given[i] + more
            rest = rest - more
    return np.array(given)


def noise(stream_key, extent, scale, most, pieces=(), held_as=jnp.bfloat16):
    result = scale * jax.random.normal(stream_key, extent, jnp.float32)
    if pieces:
        result = result * steps_of(stream_key, extent, pieces, -0.22, 0.18)
    return jnp.clip(result, -most, most).astype(held_as)


def gaussian_with(stream_key, extent, deviation, bound, split, heavy, kind=jnp.bfloat16):
    result = deviation * jax.random.normal(stream_key, extent, jnp.float32)
    if split:
        result = result * steps_of(stream_key, extent, split, -0.22, 0.18)
    return jnp.clip(with_spikes(result, jax.random.fold_in(stream_key, 3), *heavy), -bound, bound).astype(kind)


def setup_inputs(seed: int = 0) -> dict:
    keys = jax.random.split(jax.random.key(seed), 8)
    tokens = gaussian_with(keys[0], (TOKENS, D), 1.0, 6.0, ((0, 32),), (0, 1, 32, 2.75))
    out_grad = gaussian_with(keys[1], (TOKENS, D), 1.0, 6.0, ((0, 32),), (0, 1, 32, 2.75))
    expert_ids_keys = jax.random.split(jax.random.fold_in(keys[2], 1), TOKENS // TOK_DEV)
    expert_ids_turns = jax.random.permutation(jax.random.fold_in(keys[2], 3), TOKENS // TOK_DEV)
    expert_ids = jax.vmap(lambda own, number: routed_block(jax.random.fold_in(keys[2], 2), own, number, TOK_DEV, EXPERTS_WIN, TOP_WIN, CAP, 2))(expert_ids_keys, expert_ids_turns).reshape((TOKENS, TOP_WIN))
    route_weight = jnp.clip(jnp.exp(math.log(1.0) - 2.306499 * jax.random.uniform(keys[3], (TOKENS, TOP_WIN), jnp.float32) ** steps_of(keys[3], (TOKENS, TOP_WIN), ((0, 32),), -0.2, 0.2)), 0.099609375, 1.0).astype(jnp.bfloat16)
    w_gate = noise(keys[4], (EXPERTS_WIN, D, FF), D ** -0.5, 0.125, ((0, 8), (1, 4)))
    w_up = noise(keys[5], (EXPERTS_WIN, D, FF), D ** -0.5, 0.125, ((0, 8), (1, 4)))
    w_down = noise(keys[6], (EXPERTS_WIN, FF, D), FF ** -0.5, 0.21875, ((0, 8), (2, 4)))
    return {"tokens": tokens, "out_grad": out_grad, "expert_ids": expert_ids, "route_weight": route_weight, "w_gate": w_gate, "w_up": w_up, "w_down": w_down}


def reference(tokens, out_grad, expert_ids, route_weight, w_gate, w_up, w_down):
    group_routes = TOK_DEV * N_EXPERT * TOP_WIN
    row_limit = N_EXPERT * CAP
    all_routes = group_routes * N_DP
    all_tokens = TOK_DEV * N_EXPERT * N_DP
    flat_ids = expert_ids.reshape(N_DP, group_routes)
    flat_weights = route_weight.reshape(all_routes)

    def one_group(expert_index, group_index):
        picked = jnp.nonzero(flat_ids[group_index] == expert_index, size=row_limit, fill_value=-1)[0]
        valid = picked >= 0
        route_index = (group_index * group_routes + jnp.maximum(picked, 0)).astype(jnp.int32)
        token_index = (route_index // TOP_WIN).astype(jnp.int32)
        rows_in = jnp.where(valid[:, None], tokens[token_index], jnp.zeros((), tokens.dtype))
        rows_grad = jnp.where(valid[:, None], out_grad[token_index], jnp.zeros((), out_grad.dtype))
        weights = jnp.where(valid, flat_weights[route_index], jnp.zeros((), route_weight.dtype))
        gate_w = w_gate[expert_index]
        up_w = w_up[expert_index]
        down_w = w_down[expert_index]
        gate_value = jnp.dot(rows_in, gate_w, preferred_element_type=jnp.float32)
        up_value = jnp.dot(rows_in, up_w, preferred_element_type=jnp.float32)
        sigmoid_gate = jax.nn.sigmoid(gate_value)
        activated = gate_value * sigmoid_gate
        hidden = (activated * up_value).astype(jnp.bfloat16)
        expert_out = jnp.dot(hidden, down_w, preferred_element_type=jnp.float32)
        route_dot = jnp.sum(expert_out * rows_grad.astype(jnp.float32), axis=1).astype(jnp.bfloat16)
        scaled = (weights.astype(jnp.float32)[:, None] * rows_grad.astype(jnp.float32)).astype(jnp.bfloat16)
        hidden_grad = jnp.dot(scaled, down_w.T, preferred_element_type=jnp.float32)
        gate_delta = (hidden_grad * up_value * sigmoid_gate * (1.0 + gate_value * (1.0 - sigmoid_gate))).astype(jnp.bfloat16)
        up_delta = (hidden_grad * activated).astype(jnp.bfloat16)
        input_grad = (jnp.dot(gate_delta, gate_w.T, preferred_element_type=jnp.float32)
                      + jnp.dot(up_delta, up_w.T, preferred_element_type=jnp.float32)).astype(jnp.bfloat16)
        gate_part = jnp.dot(rows_in.T, gate_delta, preferred_element_type=jnp.float32).astype(jnp.bfloat16)
        up_part = jnp.dot(rows_in.T, up_delta, preferred_element_type=jnp.float32).astype(jnp.bfloat16)
        down_part = jnp.dot(hidden.T, scaled, preferred_element_type=jnp.float32).astype(jnp.bfloat16)
        target = jnp.where(valid, route_index, all_routes).astype(jnp.int32)
        return target, input_grad, route_dot, gate_part, up_part, down_part

    def one_expert(totals, expert_index):
        route_rows, route_dots = totals

        def group_step(group_index):
            return one_group(expert_index, group_index)

        target, input_grad, route_dot, gate_part, up_part, down_part = lax.map(group_step, jnp.arange(N_DP, dtype=jnp.int32))
        flat_target = target.reshape(-1)
        route_rows = route_rows.at[flat_target].set(input_grad.reshape(-1, D), mode="drop")
        route_dots = route_dots.at[flat_target].set(route_dot.reshape(-1), mode="drop")
        gate_sum = jnp.sum(gate_part.astype(jnp.float32), axis=0).astype(jnp.bfloat16)
        up_sum = jnp.sum(up_part.astype(jnp.float32), axis=0).astype(jnp.bfloat16)
        down_sum = jnp.sum(down_part.astype(jnp.float32), axis=0).astype(jnp.bfloat16)
        return (route_rows, route_dots), (gate_sum, up_sum, down_sum)

    start_rows = (jnp.zeros((all_routes, D), jnp.bfloat16), jnp.zeros((all_routes,), jnp.bfloat16))
    finals, grads = lax.scan(one_expert, start_rows, jnp.arange(EXPERTS_WIN, dtype=jnp.int32))
    route_rows, route_dots = finals
    gate_grad, up_grad, down_grad = grads
    token_grad = jnp.sum(route_rows.astype(jnp.float32).reshape(all_tokens, TOP_WIN, D), axis=1).astype(jnp.bfloat16)
    route_grad = route_dots.reshape(all_tokens, TOP_WIN)
    return (token_grad, route_grad, gate_grad, up_grad, down_grad)
```

```python
import jax
import jax.numpy as jnp
from jax import lax
from jax.sharding import PartitionSpec as P

BF16 = jnp.bfloat16
F32 = jnp.float32


def halving_order(array, axis_name, bits):
    size = lax.axis_size(axis_name)
    me = lax.axis_index(axis_name)
    levels = size.bit_length() - 1
    kept = array.reshape((2,) * levels + array.shape[1:])
    alive = list(range(levels - 1, -1, -1))
    for bit in bits:
        at = alive.index(bit)
        mine = (me >> bit) & 1
        send = lax.dynamic_index_in_dim(kept, 1 - mine, axis=at, keepdims=False)
        keep = lax.dynamic_index_in_dim(kept, mine, axis=at, keepdims=False)
        got = lax.ppermute(send, axis_name, [(i, i ^ (1 << bit)) for i in range(size)])
        kept = (keep.astype(F32) + got.astype(F32)).astype(BF16)
        alive.pop(at)
    return kept


def reduce_blocks(parts, axis_name):
    size = lax.axis_size(axis_name)
    if size == 1:
        return parts[0]
    if size & (size - 1):
        return lax.psum_scatter(parts, axis_name, scatter_dimension=0, tiled=False)
    bits = list(range(size.bit_length() - 1))
    half = parts.shape[1] // 2
    low = halving_order(parts[:, :half], axis_name, bits)
    high = halving_order(parts[:, half:], axis_name, bits[::-1])
    return jnp.concatenate([low, high], axis=0)


def dot(a, b, dims):
    return lax.dot_general(a, b, (dims, ((), ())), preferred_element_type=F32)


def on_device(tokens, out_grad, expert_ids, route_weight, w_gate, w_up, w_down):
    tok_count, width = tokens.shape
    route_count = expert_ids.shape[1]
    ranks = lax.axis_size("expert")
    groups = lax.axis_size("dp")
    assert w_gate.shape[0] == 1
    ff = w_gate.shape[2]
    experts = ranks
    capacity = 3 * tok_count * route_count // (2 * experts)
    padded = -(-capacity // 8) * 8
    first = -(-padded // 16) * 8
    chunks = ((0, first), (first, padded - first))

    full_gate = lax.all_gather(w_gate[0], "dp", axis=0, tiled=True)
    full_up = lax.all_gather(w_up[0], "dp", axis=0, tiled=True)
    full_down = lax.all_gather(w_down[0], "dp", axis=1, tiled=True)

    named = expert_ids.T[:, None, :] == jnp.arange(experts, dtype=jnp.int32)[None, :, None]
    weights = route_weight.T.astype(F32)
    member = jnp.any(named, axis=0)
    before = (
        jnp.arange(tok_count)[:, None] < jnp.arange(tok_count)[None, :]
    ).astype(BF16)
    place = dot(member.astype(BF16), before, ((1,), (0,))).astype(jnp.int32)
    place = jnp.where(member, place, -1)
    member_weight = jnp.sum(jnp.where(named, weights[:, None, :], 0.0), axis=0)

    picks, sent = [], []
    for start, rows in chunks:
        slots = start + jnp.arange(rows, dtype=jnp.int32)
        pick = place[:, None, :] == slots[None, :, None]
        select = pick.astype(BF16).reshape(experts * rows, tok_count)
        scale = jnp.where(pick, member_weight[:, None, :], 0.0).astype(BF16)
        scale = scale.reshape(experts * rows, tok_count)
        rows_in = dot(select, tokens, ((1,), (0,))).astype(BF16)
        rows_grad = dot(scale, out_grad, ((1,), (0,))).astype(BF16)
        picks.append(pick)
        sent.append((rows_in.reshape(experts, rows, width), rows_grad.reshape(experts, rows, width)))

    gate_term = up_term = down_term = None
    back_rows, back_dots = [], []
    for (start, rows), (rows_in, rows_grad) in zip(chunks, sent):
        x = lax.all_to_all(rows_in, "expert", 0, 0, tiled=True).reshape(experts * rows, width)
        s = lax.all_to_all(rows_grad, "expert", 0, 0, tiled=True).reshape(experts * rows, width)
        gate_value = dot(x, full_gate, ((1,), (0,)))
        up_value = dot(x, full_up, ((1,), (0,)))
        sig = jax.nn.sigmoid(gate_value)
        act = gate_value * sig
        hidden = (act * up_value).astype(BF16)
        hidden_grad = dot(s, full_down, ((1,), (1,)))
        down = dot(hidden, s, ((0,), (0,)))
        down_term = down if down_term is None else down_term + down
        dots = jnp.sum(hidden.astype(F32) * hidden_grad, axis=1)
        gate_delta = (hidden_grad * up_value * sig * (1.0 + gate_value * (1.0 - sig))).astype(BF16)
        up_delta = (hidden_grad * act).astype(BF16)
        gate = dot(x, gate_delta, ((0,), (0,)))
        up = dot(x, up_delta, ((0,), (0,)))
        gate_term = gate if gate_term is None else gate_term + gate
        up_term = up if up_term is None else up_term + up
        grad = (
            dot(gate_delta, full_gate, ((1,), (1,))) + dot(up_delta, full_up, ((1,), (1,)))
        ).astype(BF16)
        back_rows.append(
            lax.all_to_all(grad.reshape(experts, rows, width), "expert", 0, 0, tiled=True)
        )
        back_dots.append(dots.reshape(experts, rows))

    down_parts = down_term.astype(BF16)
    down_parts = jnp.stack(jnp.split(down_parts, groups, axis=1), axis=0)
    down_grad = reduce_blocks(down_parts, "dp")
    gate_grad = reduce_blocks(gate_term.astype(BF16).reshape(groups, -1, ff), "dp")
    up_grad = reduce_blocks(up_term.astype(BF16).reshape(groups, -1, ff), "dp")

    all_dots = jnp.concatenate(back_dots, axis=1)
    all_dots = lax.all_to_all(all_dots, "expert", 0, 0, tiled=True)
    token_sum = None
    dot_of = 0.0
    for (start, rows), pick, got in zip(chunks, picks, back_rows):
        select = pick.astype(BF16).reshape(experts * rows, tok_count)
        part = dot(select, got.reshape(experts * rows, width), ((0,), (0,)))
        token_sum = part if token_sum is None else token_sum + part
        dot_of = dot_of + jnp.sum(
            jnp.where(pick, all_dots[:, start : start + rows, None], 0.0), axis=1
        )
    token_grad = token_sum.astype(BF16)
    chosen = jnp.sum(jnp.where(named, dot_of[None], 0.0), axis=1)
    route_grad = (chosen / weights).T.astype(BF16)
    return (token_grad, route_grad, gate_grad[None], up_grad[None], down_grad[None])


def solution(mesh):
    placed = (
        P(("dp", "expert"), None),
        P(("dp", "expert"), None),
        P(("dp", "expert"), None),
        P(("dp", "expert"), None),
        P("expert", "dp", None),
        P("expert", "dp", None),
        P("expert", None, "dp"),
    )
    return jax.shard_map(
        on_device,
        mesh=mesh,
        in_specs=placed,
        out_specs=(
            P(("dp", "expert"), None),
            P(("dp", "expert"), None),
            P("expert", "dp", None),
            P("expert", "dp", None),
            P("expert", None, "dp"),
        ),
        check_vma=False,
    )
```
